128 devices in a mesh: grp: 32 (over y, z_hi, x), sub: 4 (over z_lo, core).
Axes of the slice: x: 4, y: 4, z: 4 (z_hi: 2, z_lo: 2; z = z_hi * 2 + z_lo), core: 2. Of those that a mesh axis runs over, the one named last changes fastest.
Arguments:
- master: float32 [16384, 3584], P(('grp', 'sub')), may hold values from -120 to 120
- moment_one: float32 [16384, 3584], P(('grp', 'sub')), may hold values from -6 to 6
- moment_two: float32 [16384, 3584], P(('grp', 'sub')), may hold values from 0.01 to 4
- gradient: float32 [16384, 3584], P(('grp', 'sub')), may hold values from -120 to 120
- partner: int32 [128], replicated, may hold values from 0 to 127, each once
- tensor_of_row: int32 [16384], replicated, may hold values from 0 to 7, never falling along the last dimension, each value on 1 to 4096 neighbouring positions
Outputs:
- new_master: float32 [16384, 3584], P(('grp', 'sub'))
- new_moment_one: float32 [16384, 3584], P(('grp', 'sub'))
- new_moment_two: float32 [16384, 3584], P(('grp', 'sub'))
The draws below stay inside these ranges and needn't reach their ends.
Inputs may be any that keep to these rules, and one draw needn't show every extreme that they name: partner[n] is the device of new rank n; every device holds exactly one rank. `tensor_of_row`: tensor numbers never fall along the rows; each of the 8 tensors has one or more rows.
All inputs are finite; a program needn't handle non-finite values.
Results may differ from the reference program's by a relative error of at most 0.00007.
Values sent between devices are 32-bit elements; how exact they have to be, the bound alone decides.
A program may use at most 128 MiB of HBM per device.

```python
import math
import jax
import jax.numpy as jnp
import numpy as np
from jax import lax

W = 3584
ROWS_DEV = 128
LAYERS = 8
NDEV = 128
ROWS = 16384
BLOCK = 1


def scale_field(key, trend_pos):
    key_row, key_col = jax.random.split(key, 2)
    row_scale = jnp.exp(jax.random.uniform(key_row, (ROWS, 1), jnp.float32, 0.0, math.log(10.0)))
    col_scale = jnp.exp(jax.random.uniform(key_col, (1, W), jnp.float32, 0.0, math.log(10.0)))
    trend = jnp.power(3.0, trend_pos.astype(jnp.float32) / max(NDEV - 1, 1))
    return row_scale * col_scale * trend[:, None] / 15.0


def draw_master(key, part):
    key = jax.random.fold_in(key, 11)
    key_scale, key_noise = jax.random.split(key, 2)
    row_index = jnp.arange(ROWS, dtype=jnp.int32)
    trend_pos = row_index % ROWS_DEV // BLOCK
    noise = jax.random.normal(key_noise, (ROWS, W), jnp.float32)
    noise = jnp.clip(noise, -6.0, 6.0)
    return noise * scale_field(key_scale, trend_pos)


def draw_gradient(key, part):
    key = jax.random.fold_in(key, 23)
    key_scale, key_noise = jax.random.split(key, 2)
    row_index = jnp.arange(ROWS, dtype=jnp.int32)
    trend_pos = row_index // ROWS_DEV
    noise = jax.random.normal(key_noise, (ROWS, W), jnp.float32)
    noise = jnp.clip(noise, -6.0, 6.0)
    return noise * scale_field(key_scale, trend_pos)


def steps_of(rng, dims, pieces, smallest, top_value):
    gain, own = 1.0, jax.random.fold_in(rng, 6)
    for dim, shards_of in pieces:
        steps = jnp.exp(jax.random.uniform(jax.random.fold_in(own, dim), (shards_of,), jnp.float32, smallest / len(pieces), top_value / len(pieces)))
        gain = gain * jnp.repeat(steps, dims[dim] // shards_of).reshape([-1 if axis == dim else 1 for axis in range(len(dims))])
    return gain


def profile(count, total, bound, slope):
    loads = [(1 << 20) // math.isqrt(standing ** slope) + 1 for standing in range(2, count + 1)]
    surplus, given = total - bound - (count - 1), [1] * (count - 1)
    while surplus > 0:
        candidates = [i for i in range(count - 1) if given[i] < bound]
        pool, remaining = sum([loads[i] for i in candidates]), surplus
        for i in candidates:
            extra = min(bound - given[i], max(1, remaining * loads[i] // pool), surplus)
            given[i] = given[i] + extra
            surplus = surplus - extra
    return np.array([bound] + given)


def ragged_sizes(rng, number_of, total, bound, slope):
    if number_of == 2:
        one = jax.random.randint(rng, (), max(1, total - bound), min(bound, total - 1) + 1)
        return jnp.stack([one, total - one])
    sizes = jnp.asarray(profile(number_of, total, bound, slope), jnp.int32)
    twos = (number_of - 1) // 2
    donor, sink = sizes[1:1 + 2 * twos:2], sizes[2:2 + 2 * twos:2]
    slack = jnp.minimum(donor - 1, bound - sink)
    shifted = jax.random.randint(jax.random.fold_in(rng, 1), (twos,), 0, 1 << 20) % (slack + 1)
    sizes = sizes.at[1:1 + 2 * twos:2].set(donor - shifted).at[2:2 + 2 * twos:2].set(sink + shifted)
    return sizes[jax.random.permutation(jax.random.fold_in(rng, 2), number_of)]


def gaussian(own_key, extent, spread, bound, cuts=(), kind=jnp.bfloat16):
    entries = jax.random.normal(own_key, extent, jnp.float32) * spread
    if len(cuts) > 0:
        entries = steps_of(own_key, extent, cuts, -0.22, 0.18) * entries
    return jnp.clip(entries, min=-bound, max=bound).astype(kind)


def setup_inputs(seed: int = 0) -> dict:
    keys = jax.random.split(jax.random.key(seed), 7)
    return {
        "master": draw_master(jax.random.fold_in(keys[6], 71), 0),
        "moment_one": gaussian(keys[1], (ROWS, W), 1.0, 6.0, ((0, 128),), jnp.float32),
        "moment_two": jnp.clip(jnp.exp(math.log(4.0) - 5.9914646 * jax.random.uniform(keys[2], (ROWS, W), jnp.float32) ** steps_of(keys[2], (ROWS, W), ((0, 128),), -0.2, 0.2)), 0.01, 4.0),
        "gradient": draw_gradient(jax.random.fold_in(keys[6], 71), 0),
        "partner": jax.random.permutation(keys[4], NDEV).astype(jnp.int32),
        "tensor_of_row": jnp.searchsorted(jnp.cumsum(ragged_sizes(keys[5], LAYERS, ROWS, 2 * ROWS // LAYERS, 1)), jnp.arange(ROWS), side="right").astype(jnp.int32),
    }


beta_one = 0.9
beta_two = 0.999
step_count = 10
adam_eps = 1e-06
trust_eps = 1e-06
learn_rate = 0.05
decay_rate = 0.01

def reference(master, moment_one, moment_two, gradient, partner, tensor_of_row):
    total_rows = master.shape[0]
    row_index = jnp.arange(total_rows, dtype=jnp.int32)
    owner = row_index // ROWS_DEV
    inside = row_index % ROWS_DEV
    rank = inside // BLOCK
    offset = inside % BLOCK
    place = (partner[rank] * ROWS_DEV + owner * BLOCK + offset).astype(jnp.int32)
    grad_rows = gradient[place]
    first = beta_one * moment_one + (1.0 - beta_one) * grad_rows
    second = beta_two * moment_two + (1.0 - beta_two) * grad_rows * grad_rows
    correct_one = 1.0 - beta_one ** step_count
    correct_two = 1.0 - beta_two ** step_count
    update = first / correct_one / (jnp.sqrt(second / correct_two) + adam_eps) + decay_rate * master
    weight_sq = jax.ops.segment_sum(lax.optimization_barrier(jnp.sum(master * master, axis=1)), tensor_of_row, num_segments=LAYERS)
    update_sq = jax.ops.segment_sum(lax.optimization_barrier(jnp.sum(update * update, axis=1)), tensor_of_row, num_segments=LAYERS)
    ratio = jnp.sqrt(weight_sq) / (jnp.sqrt(update_sq) + trust_eps)
    row_ratio = ratio[tensor_of_row]
    fresh = master - learn_rate * row_ratio[:, None] * update

    def settle(values):
        return jnp.zeros_like(values).at[place].set(values)
    return (settle(fresh), settle(first), settle(second))
```

```python
import functools

import jax
import jax.numpy as jnp
from jax import lax
from jax.experimental import pallas as pl
from jax.experimental.pallas import tpu as pltpu
from jax.sharding import Mesh
from jax.sharding import PartitionSpec as P

LAYERS = 8
AXES = ("grp_0", "grp_1", "grp_2", "sub_0", "sub_1")
LOGICAL = pl.DeviceIdType.LOGICAL
STRIDE = 37
LANES = 128
GROUP = 8


beta_one = 0.9
beta_two = 0.999
step_count = 10
adam_eps = 1e-06
trust_eps = 1e-06
learn_rate = 0.05
decay_rate = 0.01


def own_place():
    y = lax.axis_index("grp_0")
    z = lax.axis_index("grp_1") * 2 + lax.axis_index("sub_0")
    x = lax.axis_index("grp_2")
    core = lax.axis_index("sub_1")
    return x, y, z, core


def number_of(x, y, z, core):
    return (((y * 2 + z // 2) * 4 + x) * 2 + z % 2) * 2 + core


def exchange_kernel(
    inverse, partner, row_tensor, master, moment_one, moment_two, gradient,
    weights, update, first, second, row_ratio,
    source, sending, spare, ids, partial, totals,
    load_sem, grad_sem, send_sem, recv_sem, total_send_sem, total_recv_sem,
):
    devices, width = weights.shape
    blocks = devices // GROUP
    x, y, z, core = own_place()
    me = number_of(x, y, z, core)
    arrived = (weights, first, second)

    def target(step):
        offset = (step * STRIDE) % devices
        return number_of(
            (x + offset // 32) % 4, (y + offset // 8 % 4) % 4, (z + offset // 2 % 4) % 4, (core + offset % 2) % 2
        )

    loads = [
        pltpu.make_async_copy(array, source.at[k], load_sem.at[k])
        for k, array in enumerate((master, moment_one, moment_two))
    ]
    for load in loads:
        load.start()
    grad_load = pltpu.make_async_copy(gradient, update, grad_sem)
    grad_load.start()

    barrier = pltpu.get_barrier_semaphore()

    def greet(step, carry):
        pl.semaphore_signal(barrier, inc=1, device_id=(me + step) % devices, device_id_type=LOGICAL)
        return carry

    lax.fori_loop(1, devices, greet, 0)

    held = lax.broadcasted_iota(jnp.int32, (devices, devices), 1)
    mine = jnp.where(partner[...] == me, row_tensor[...] + held * 0, 0)
    ids[...] = jnp.broadcast_to(jnp.sum(mine, axis=1, keepdims=True), (devices, LANES))

    for load in loads:
        load.wait()

    def pick(step):
        row = inverse[target(step)]
        for k in range(3):
            sending[k, pl.ds(step, 1), :] = source[k, pl.ds(row, 1), :]

    def send(step):
        there = target(step)
        for k in range(3):
            pltpu.make_async_remote_copy(
                src_ref=sending.at[k, pl.ds(step, 1)],
                dst_ref=arrived[k].at[pl.ds(me, 1)],
                send_sem=send_sem,
                recv_sem=recv_sem.at[me // GROUP],
                device_id=there,
                device_id_type=LOGICAL,
            ).start()

    for step in range(GROUP):
        pick(step)
    pl.semaphore_wait(barrier, devices - 1)

    def keep():
        for k in range(3):
            pltpu.make_async_copy(
                sending.at[k, pl.ds(0, 1)], arrived[k].at[pl.ds(me, 1)], recv_sem.at[me // GROUP]
            ).start()
            pltpu.make_async_copy(sending.at[k, pl.ds(0, 1)], spare.at[k, pl.ds(0, 1)], send_sem).start()

    def pick_group(group):
        for j in range(GROUP):
            pick(group * GROUP + j)

    pick_group(1)
    keep()
    for step in range(1, GROUP):
        send(step)

    def round_of(group, carry):
        pick_group(group + 1)
        for j in range(GROUP):
            send(group * GROUP + j)
        return carry

    lax.fori_loop(1, blocks - 1, round_of, 0)
    for j in range(GROUP):
        send((blocks - 1) * GROUP + j)

    grad_load.wait()
    scale_one = 1.0 / (1.0 - beta_one**step_count)
    scale_two = 1.0 / (1.0 - beta_two**step_count)

    def compute(block, sums):
        pltpu.make_async_copy(
            sending.at[0, pl.ds(0, 3 * GROUP)], source.at[0, pl.ds(0, 3 * GROUP)], recv_sem.at[block]
        ).wait()
        rows = pl.ds(pl.multiple_of(block * GROUP, GROUP), GROUP)
        row_update = jnp.zeros((GROUP, LANES), jnp.float32)
        row_weight = jnp.zeros((GROUP, LANES), jnp.float32)
        for lane in range(0, width, LANES):
            cols = pl.ds(lane, LANES)
            grad = update[rows, cols]
            weight = weights[rows, cols]
            new_first = beta_one * first[rows, cols] + (1.0 - beta_one) * grad
            new_second = beta_two * second[rows, cols] + (1.0 - beta_two) * grad * grad
            step = (new_first * scale_one) / (jnp.sqrt(new_second * scale_two) + adam_eps) + decay_rate * weight
            first[rows, cols] = new_first
            second[rows, cols] = new_second
            update[rows, cols] = step
            row_update += step * step
            row_weight += weight * weight
        tensor = ids[rows, :]
        return tuple(
            (
                sums[t][0] + jnp.where(tensor == t, row_update, 0.0),
                sums[t][1] + jnp.where(tensor == t, row_weight, 0.0),
            )
            for t in range(LAYERS)
        )

    zero = jnp.zeros((GROUP, LANES), jnp.float32)
    sums = lax.fori_loop(0, blocks, compute, tuple((zero, zero) for _ in range(LAYERS)))

    lane_id = lax.broadcasted_iota(jnp.int32, (1, LANES), 1)
    packed = jnp.zeros((1, LANES), jnp.float32)
    for t in range(LAYERS):
        for part in range(2):
            packed = jnp.where(lane_id == t + LAYERS * part, jnp.sum(sums[t][part]), packed)
    partial[...] = jnp.broadcast_to(packed, (GROUP, LANES))

    def tell(step, carry):
        pltpu.make_async_remote_copy(
            src_ref=partial.at[pl.ds(0, 1)],
            dst_ref=totals.at[pl.ds(me, 1)],
            send_sem=total_send_sem,
            recv_sem=total_recv_sem,
            device_id=target(step),
            device_id_type=LOGICAL,
        ).start()
        return carry

    lax.fori_loop(1, devices, tell, 0)
    pltpu.make_async_copy(partial.at[pl.ds(0, 1)], totals.at[pl.ds(me, 1)], total_recv_sem).start()
    pltpu.make_async_copy(partial.at[pl.ds(0, 1)], spare.at[0, pl.ds(1, 1), pl.ds(0, LANES)], total_send_sem).start()
    pltpu.make_async_copy(totals, totals, total_recv_sem).wait()
    summed = jnp.sum(totals[...], axis=0, keepdims=True)
    ratio = jnp.sqrt(pltpu.roll(summed, LANES - LAYERS, 1)) / (jnp.sqrt(summed) + trust_eps)
    hot = lax.broadcasted_iota(jnp.int32, (devices, LANES), 1) == ids[...]
    per_row = jnp.sum(jnp.where(hot, ratio, 0.0), axis=1, keepdims=True)
    row_ratio[...] = jnp.broadcast_to(per_row, (devices, LANES))

    pltpu.make_async_copy(sending, source, send_sem).wait()
    pltpu.make_async_copy(totals, totals, total_send_sem).wait()


def finish_kernel(weights, update, first, second, row_ratio, new_master, new_one, new_two, fresh, sem_one, sem_two, sem_fresh):
    rows, width = weights.shape
    one = pltpu.make_async_copy(first, new_one, sem_one)
    two = pltpu.make_async_copy(second, new_two, sem_two)
    one.start()
    two.start()
    chunk = 32
    writes = []
    for index in range(rows // chunk):
        at = pl.ds(index * chunk, chunk)
        scale = learn_rate * row_ratio[at, :]
        for lane in range(0, width, LANES):
            cols = pl.ds(lane, LANES)
            fresh[at, cols] = weights[at, cols] - scale * update[at, cols]
        writes.append(pltpu.make_async_copy(fresh.at[at], new_master.at[at], sem_fresh.at[index]))
        writes[-1].start()
    for write in writes:
        write.wait()
    one.wait()
    two.wait()


def local(master, moment_one, moment_two, gradient, partner, tensor_of_row):
    rows_dev, width = master.shape
    devices = partner.shape[0]
    numbers = jnp.arange(devices, dtype=jnp.int32)
    inverse = jnp.sum(jnp.where(partner[None, :] == numbers[:, None], numbers[None, :], 0), axis=1)
    vmem = pl.BlockSpec(memory_space=pltpu.VMEM)
    hbm = pl.BlockSpec(memory_space=pltpu.HBM)
    smem = pl.BlockSpec(memory_space=pltpu.SMEM)
    block = pltpu.VMEM((rows_dev, width), jnp.float32)
    stack = pltpu.VMEM((3, rows_dev, width), jnp.float32)
    dma = pltpu.SemaphoreType.DMA
    weights, update, first, second, row_ratio = pl.pallas_call(
        exchange_kernel,
        out_shape=(block, block, block, block, pltpu.VMEM((rows_dev, LANES), jnp.float32)),
        in_specs=[smem, vmem, vmem, hbm, hbm, hbm, hbm],
        out_specs=(vmem,) * 5,
        scratch_shapes=[
            stack,
            stack,
            pltpu.VMEM((3, GROUP, width), jnp.float32),
            pltpu.VMEM((rows_dev, LANES), jnp.int32),
            pltpu.VMEM((GROUP, LANES), jnp.float32),
            pltpu.VMEM((devices, LANES), jnp.float32),
            dma((3,)),
            dma,
            dma,
            dma((devices // GROUP,)),
            dma,
            dma,
        ],
        compiler_params=pltpu.CompilerParams(
            collective_id=0, has_side_effects=True, vmem_limit_bytes=24 * 1024 * 1024
        ),
        name="exchange",
    )(inverse, partner.reshape(1, devices), tensor_of_row.reshape(devices, devices), master, moment_one, moment_two, gradient)
    whole = jax.ShapeDtypeStruct((rows_dev, width), jnp.float32)
    return pl.pallas_call(
        finish_kernel,
        out_shape=(whole,) * 3,
        in_specs=[vmem] * 5,
        out_specs=(hbm,) * 3,
        scratch_shapes=[block, dma, dma, dma((4,))],
        compiler_params=pltpu.CompilerParams(vmem_limit_bytes=8 * 1024 * 1024),
        name="finish",
    )(weights, update, first, second, row_ratio)


def solution(mesh):
    finer = Mesh(mesh.devices.reshape(4, 2, 4, 2, 2), AXES)
    in_specs = (P(AXES, None), P(AXES, None), P(AXES, None), P(AXES, None), P(), P())
    out_specs = (P(AXES, None), P(AXES, None), P(AXES, None))
    return jax.shard_map(local, mesh=finer, in_specs=in_specs, out_specs=out_specs, check_vma=False)
```

```python
import functools

import jax
import jax.numpy as jnp
from jax import lax
from jax.experimental import pallas as pl
from jax.experimental.pallas import tpu as pltpu
from jax.sharding import Mesh
from jax.sharding import PartitionSpec as P

LAYERS = 8
AXES = ("grp_0", "grp_1", "grp_2", "sub_0", "sub_1")
LOGICAL = pl.DeviceIdType.LOGICAL
STRIDE = 37
LANES = 128
GROUP = 8


beta_one = 0.9
beta_two = 0.999
step_count = 10
adam_eps = 1e-06
trust_eps = 1e-06
learn_rate = 0.05
decay_rate = 0.01


def own_place():
    y = lax.axis_index("grp_0")
    z = lax.axis_index("grp_1") * 2 + lax.axis_index("sub_0")
    x = lax.axis_index("grp_2")
    core = lax.axis_index("sub_1")
    return x, y, z, core


def number_of(x, y, z, core):
    return (((y * 2 + z // 2) * 4 + x) * 2 + z % 2) * 2 + core


def exchange_kernel(
    partner, tensor_of_row, master, moment_one, moment_two, gradient,
    weights, update, first, second, row_ratio,
    source, sending, spare, row_tensor, ids, partner_row, inverse_row, inverse, partial, totals,
    load_sem, partner_sem, tensor_sem, grad_sem, send_sem, recv_sem, total_send_sem, total_recv_sem,
):
    devices, width = weights.shape
    blocks = devices // GROUP
    x, y, z, core = own_place()
    me = number_of(x, y, z, core)
    arrived = (weights, first, second)

    def target(step):
        offset = (step * STRIDE) % devices
        return number_of(
            (x + offset // 32) % 4, (y + offset // 8 % 4) % 4, (z + offset // 2 % 4) % 4, (core + offset % 2) % 2
        )

    partner_load = pltpu.make_async_copy(partner, partner_row, partner_sem)
    partner_load.start()
    loads = [
        pltpu.make_async_copy(array, source.at[k], load_sem.at[k])
        for k, array in enumerate((master, moment_one, moment_two))
    ]
    for load in loads:
        load.start()
    grad_load = pltpu.make_async_copy(gradient, update, grad_sem)
    grad_load.start()
    tensor_load = pltpu.make_async_copy(tensor_of_row, row_tensor, tensor_sem)
    tensor_load.start()

    barrier = pltpu.get_barrier_semaphore()

    def greet(step, carry):
        pl.semaphore_signal(barrier, inc=1, device_id=(me + step) % devices, device_id_type=LOGICAL)
        return carry

    lax.fori_loop(1, devices, greet, 0)

    down = lax.broadcasted_iota(jnp.int32, (devices, devices), 0)
    across = lax.broadcasted_iota(jnp.int32, (devices, devices), 1)
    partner_load.wait()
    places = jnp.broadcast_to(partner_row[...], (devices, devices))
    rank_of = jnp.sum(jnp.where(places == down, across, 0), axis=1, keepdims=True)
    turned = jnp.sum(jnp.where(down == across, rank_of, 0), axis=0, keepdims=True)
    inverse_row[...] = jnp.broadcast_to(turned, (GROUP, devices))
    inverse_move = pltpu.make_async_copy(inverse_row.at[pl.ds(0, 1)], inverse, partner_sem)
    inverse_move.start()
    tensor_load.wait()
    mine = jnp.where(places == me, row_tensor[...], 0)
    ids[...] = jnp.broadcast_to(jnp.sum(mine, axis=1, keepdims=True), (devices, LANES))
    inverse_move.wait()

    for load in loads:
        load.wait()

    def pick(step):
        row = inverse[0, target(step)] & (devices - 1)
        for k in range(3):
            sending[k, pl.ds(step, 1), :] = source[k, pl.ds(row, 1), :]

    def send(step):
        there = target(step)
        for k in range(3):
            pltpu.make_async_remote_copy(
                src_ref=sending.at[k, pl.ds(step, 1)],
                dst_ref=arrived[k].at[pl.ds(me, 1)],
                send_sem=send_sem,
                recv_sem=recv_sem.at[me // GROUP],
                device_id=there,
                device_id_type=LOGICAL,
            ).start()

    for step in range(GROUP):
        pick(step)
    pl.semaphore_wait(barrier, devices - 1)

    def keep():
        for k in range(3):
            pltpu.make_async_copy(
                sending.at[k, pl.ds(0, 1)], arrived[k].at[pl.ds(me, 1)], recv_sem.at[me // GROUP]
            ).start()
            pltpu.make_async_copy(sending.at[k, pl.ds(0, 1)], spare.at[k, pl.ds(0, 1)], send_sem).start()

    def pick_group(group):
        for j in range(GROUP):
            pick(group * GROUP + j)

    pick_group(1)
    keep()
    for step in range(1, GROUP):
        send(step)

    def round_of(group, carry):
        pick_group(group + 1)
        for j in range(GROUP):
            send(group * GROUP + j)
        return carry

    lax.fori_loop(1, blocks - 1, round_of, 0)
    for j in range(GROUP):
        send((blocks - 1) * GROUP + j)

    grad_load.wait()
    scale_one = 1.0 / (1.0 - beta_one**step_count)
    scale_two = 1.0 / (1.0 - beta_two**step_count)

    def compute(block, sums):
        pltpu.make_async_copy(
            sending.at[0, pl.ds(0, 3 * GROUP)], source.at[0, pl.ds(0, 3 * GROUP)], recv_sem.at[block]
        ).wait()
        rows = pl.ds(pl.multiple_of(block * GROUP, GROUP), GROUP)
        row_update = jnp.zeros((GROUP, LANES), jnp.float32)
        row_weight = jnp.zeros((GROUP, LANES), jnp.float32)
        for lane in range(0, width, LANES):
            cols = pl.ds(lane, LANES)
            grad = update[rows, cols]
            weight = weights[rows, cols]
            new_first = beta_one * first[rows, cols] + (1.0 - beta_one) * grad
            new_second = beta_two * second[rows, cols] + (1.0 - beta_two) * grad * grad
            step = (new_first * scale_one) / (jnp.sqrt(new_second * scale_two) + adam_eps) + decay_rate * weight
            first[rows, cols] = new_first
            second[rows, cols] = new_second
            update[rows, cols] = step
            row_update += step * step
            row_weight += weight * weight
        tensor = ids[rows, :]
        return tuple(
            (
                sums[t][0] + jnp.where(tensor == t, row_update, 0.0),
                sums[t][1] + jnp.where(tensor == t, row_weight, 0.0),
            )
            for t in range(LAYERS)
        )

    zero = jnp.zeros((GROUP, LANES), jnp.float32)
    sums = lax.fori_loop(0, blocks, compute, tuple((zero, zero) for _ in range(LAYERS)))

    lane_id = lax.broadcasted_iota(jnp.int32, (1, LANES), 1)
    packed = jnp.zeros((1, LANES), jnp.float32)
    for t in range(LAYERS):
        for part in range(2):
            packed = jnp.where(lane_id == t + LAYERS * part, jnp.sum(sums[t][part]), packed)
    partial[...] = jnp.broadcast_to(packed, (GROUP, LANES))

    def tell(step, carry):
        pltpu.make_async_remote_copy(
            src_ref=partial.at[pl.ds(0, 1)],
            dst_ref=totals.at[pl.ds(me, 1)],
            send_sem=total_send_sem,
            recv_sem=total_recv_sem,
            device_id=target(step),
            device_id_type=LOGICAL,
        ).start()
        return carry

    lax.fori_loop(1, devices, tell, 0)
    pltpu.make_async_copy(partial.at[pl.ds(0, 1)], totals.at[pl.ds(me, 1)], total_recv_sem).start()
    pltpu.make_async_copy(partial.at[pl.ds(0, 1)], spare.at[0, pl.ds(1, 1), pl.ds(0, LANES)], total_send_sem).start()
    pltpu.make_async_copy(totals, totals, total_recv_sem).wait()
    summed = jnp.sum(totals[...], axis=0, keepdims=True)
    ratio = jnp.sqrt(pltpu.roll(summed, LANES - LAYERS, 1)) / (jnp.sqrt(summed) + trust_eps)
    hot = lax.broadcasted_iota(jnp.int32, (devices, LANES), 1) == ids[...]
    per_row = jnp.sum(jnp.where(hot, ratio, 0.0), axis=1, keepdims=True)
    row_ratio[...] = jnp.broadcast_to(per_row, (devices, LANES))

    pltpu.make_async_copy(sending, source, send_sem).wait()
    pltpu.make_async_copy(totals, totals, total_send_sem).wait()


def finish_kernel(weights, update, first, second, row_ratio, new_master, new_one, new_two, fresh, sem_one, sem_two, sem_fresh):
    rows, width = weights.shape
    one = pltpu.make_async_copy(first, new_one, sem_one)
    two = pltpu.make_async_copy(second, new_two, sem_two)
    one.start()
    two.start()
    chunk = 32
    writes = []
    for index in range(rows // chunk):
        at = pl.ds(index * chunk, chunk)
        scale = learn_rate * row_ratio[at, :]
        for lane in range(0, width, LANES):
            cols = pl.ds(lane, LANES)
            fresh[at, cols] = weights[at, cols] - scale * update[at, cols]
        writes.append(pltpu.make_async_copy(fresh.at[at], new_master.at[at], sem_fresh.at[index]))
        writes[-1].start()
    for write in writes:
        write.wait()
    one.wait()
    two.wait()


def local(master, moment_one, moment_two, gradient, partner, tensor_of_row):
    rows_dev, width = master.shape
    devices = partner.shape[0]
    operands = (
        partner.reshape(1, devices), tensor_of_row.reshape(devices, devices), master, moment_one, moment_two, gradient
    )
    operands = [pltpu.with_memory_space_constraint(operand, pltpu.HBM) for operand in operands]
    vmem = pl.BlockSpec(memory_space=pltpu.VMEM)
    hbm = pl.BlockSpec(memory_space=pltpu.HBM)
    block = pltpu.VMEM((rows_dev, width), jnp.float32)
    stack = pltpu.VMEM((3, rows_dev, width), jnp.float32)
    dma = pltpu.SemaphoreType.DMA
    weights, update, first, second, row_ratio = pl.pallas_call(
        exchange_kernel,
        out_shape=(block, block, block, block, pltpu.VMEM((rows_dev, LANES), jnp.float32)),
        in_specs=[hbm] * 6,
        out_specs=(vmem,) * 5,
        scratch_shapes=[
            stack,
            stack,
            pltpu.VMEM((3, GROUP, width), jnp.float32),
            pltpu.VMEM((devices, devices), jnp.int32),
            pltpu.VMEM((rows_dev, LANES), jnp.int32),
            pltpu.VMEM((1, devices), jnp.int32),
            pltpu.VMEM((GROUP, devices), jnp.int32),
            pltpu.SMEM((1, devices), jnp.int32),
            pltpu.VMEM((GROUP, LANES), jnp.float32),
            pltpu.VMEM((devices, LANES), jnp.float32),
            dma((3,)),
            dma,
            dma,
            dma,
            dma,
            dma((devices // GROUP,)),
            dma,
            dma,
        ],
        compiler_params=pltpu.CompilerParams(
            collective_id=0, has_side_effects=True, vmem_limit_bytes=24 * 1024 * 1024
        ),
        name="exchange",
    )(*operands)
    whole = jax.ShapeDtypeStruct((rows_dev, width), jnp.float32)
    return pl.pallas_call(
        finish_kernel,
        out_shape=(whole,) * 3,
        in_specs=[vmem] * 5,
        out_specs=(hbm,) * 3,
        scratch_shapes=[block, dma, dma, dma((4,))],
        compiler_params=pltpu.CompilerParams(vmem_limit_bytes=8 * 1024 * 1024),
        name="finish",
    )(weights, update, first, second, row_ratio)


def solution(mesh):
    finer = Mesh(mesh.devices.reshape(4, 2, 4, 2, 2), AXES)
    in_specs = (P(AXES, None), P(AXES, None), P(AXES, None), P(AXES, None), P(), P())
    out_specs = (P(AXES, None), P(AXES, None), P(AXES, None))
    return jax.shard_map(local, mesh=finer, in_specs=in_specs, out_specs=out_specs, check_vma=False)
```

```python
import functools

import jax
import jax.numpy as jnp
from jax import lax
from jax.experimental import pallas as pl
from jax.experimental.pallas import tpu as pltpu
from jax.sharding import Mesh
from jax.sharding import PartitionSpec as P

LAYERS = 8
AXES = ("grp_0", "grp_1", "grp_2", "sub_0", "sub_1")
LOGICAL = pl.DeviceIdType.LOGICAL
STRIDE = 37
LANES = 128
GROUP = 8


beta_one = 0.9
beta_two = 0.999
step_count = 10
adam_eps = 1e-06
trust_eps = 1e-06
learn_rate = 0.05
decay_rate = 0.01


def own_place():
    y = lax.axis_index("grp_0")
    z = lax.axis_index("grp_1") * 2 + lax.axis_index("sub_0")
    x = lax.axis_index("grp_2")
    core = lax.axis_index("sub_1")
    return x, y, z, core


def number_of(x, y, z, core):
    return (((y * 2 + z // 2) * 4 + x) * 2 + z % 2) * 2 + core


def exchange_kernel(
    partner, tensor_of_row, master, moment_one, moment_two, gradient,
    weights, update, first, second, row_ratio,
    source, sending, spare, row_tensor, ids, partner_row, inverse_row, inverse, partial, totals,
    load_sem, partner_sem, tensor_sem, grad_sem, send_sem, recv_sem, total_send_sem, total_recv_sem,
):
    devices, width = weights.shape
    blocks = devices // GROUP
    x, y, z, core = own_place()
    me = number_of(x, y, z, core)
    arrived = (weights, first, second)

    turn = 1 - 2 * core

    def target(step):
        offset = (step * STRIDE) % devices
        return number_of(
            (x + turn * (offset // 32) + 4) % 4,
            (y + turn * (offset // 8 % 4) + 4) % 4,
            (z + turn * (offset // 2 % 4) + 4) % 4,
            (core + offset % 2) % 2,
        )

    x_part = [((x + d) % 4) * 4 for d in range(4)]
    y_part = [((y + d) % 4) * 32 for d in range(4)]
    z_part = [((z + d) % 4) // 2 * 16 + ((z + d) % 4) % 2 * 2 for d in range(4)]
    core_part = [(core + d) % 2 for d in range(2)]
    places = [(dx, dy, dz, dc) for dx in range(4) for dy in range(4) for dz in range(4) for dc in range(2)]
    places.remove((0, 0, 0, 0))
    places.sort(key=lambda d: sum(min(v, 4 - v) for v in d[:3]), reverse=True)
    others = [x_part[dx] + y_part[dy] + z_part[dz] + core_part[dc] for dx, dy, dz, dc in places]

    partner_load = pltpu.make_async_copy(partner, partner_row, partner_sem)
    partner_load.start()
    loads = [
        pltpu.make_async_copy(array, source.at[k], load_sem.at[k])
        for k, array in enumerate((master, moment_one, moment_two))
    ]
    for load in loads:
        load.start()
    grad_load = pltpu.make_async_copy(gradient, update, grad_sem)
    grad_load.start()
    tensor_load = pltpu.make_async_copy(tensor_of_row, row_tensor, tensor_sem)
    tensor_load.start()

    barrier = pltpu.get_barrier_semaphore()

    for other in others:
        pl.semaphore_signal(barrier, inc=1, device_id=other, device_id_type=LOGICAL)

    down = lax.broadcasted_iota(jnp.int32, (devices, devices), 0)
    across = lax.broadcasted_iota(jnp.int32, (devices, devices), 1)
    partner_load.wait()
    holder = jnp.broadcast_to(partner_row[...], (devices, devices))
    rank_of = jnp.sum(jnp.where(holder == down, across, 0), axis=1, keepdims=True)
    turned = jnp.sum(jnp.where(down == across, rank_of, 0), axis=0, keepdims=True)
    inverse_row[...] = jnp.broadcast_to(turned, (GROUP, devices))
    inverse_move = pltpu.make_async_copy(inverse_row.at[pl.ds(0, 1)], inverse, partner_sem)
    inverse_move.start()
    tensor_load.wait()
    mine = jnp.where(holder == me, row_tensor[...], 0)
    ids[...] = jnp.broadcast_to(jnp.sum(mine, axis=1, keepdims=True), (devices, LANES))
    inverse_move.wait()

    for load in loads:
        load.wait()

    def pick(step):
        row = inverse[0, target(step)] & (devices - 1)
        for k in range(3):
            sending[k, pl.ds(step, 1), :] = source[k, pl.ds(row, 1), :]

    def send(step):
        there = target(step)
        for k in range(3):
            pltpu.make_async_remote_copy(
                src_ref=sending.at[k, pl.ds(step, 1)],
                dst_ref=arrived[k].at[pl.ds(me, 1)],
                send_sem=send_sem,
                recv_sem=recv_sem.at[me // GROUP],
                device_id=there,
                device_id_type=LOGICAL,
            ).start()


    def keep():
        for k in range(3):
            pltpu.make_async_copy(
                sending.at[k, pl.ds(0, 1)], arrived[k].at[pl.ds(me, 1)], recv_sem.at[me // GROUP]
            ).start()
            pltpu.make_async_copy(sending.at[k, pl.ds(0, 1)], spare.at[k, pl.ds(0, 1)], send_sem).start()

    def pick_group(group):
        for j in range(GROUP):
            pick(group * GROUP + j)

    pick_group(0)
    pick_group(1)
    pl.semaphore_wait(barrier, devices - 1)
    keep()
    for step in range(1, GROUP):
        send(step)

    def round_of(group, carry):
        pick_group(group + 1)
        for j in range(GROUP):
            send(group * GROUP + j)
        return carry

    lax.fori_loop(1, blocks - 1, round_of, 0)
    for j in range(GROUP):
        send((blocks - 1) * GROUP + j)

    grad_load.wait()
    scale_one = 1.0 / (1.0 - beta_one**step_count)
    scale_two = 1.0 / (1.0 - beta_two**step_count)

    def compute(block, sums):
        pltpu.make_async_copy(
            sending.at[0, pl.ds(0, 3 * GROUP)], source.at[0, pl.ds(0, 3 * GROUP)], recv_sem.at[block]
        ).wait()
        rows = pl.ds(pl.multiple_of(block * GROUP, GROUP), GROUP)
        row_update = jnp.zeros((GROUP, LANES), jnp.float32)
        row_weight = jnp.zeros((GROUP, LANES), jnp.float32)
        for lane in range(0, width, LANES):
            cols = pl.ds(lane, LANES)
            grad = update[rows, cols]
            weight = weights[rows, cols]
            new_first = beta_one * first[rows, cols] + (1.0 - beta_one) * grad
            new_second = beta_two * second[rows, cols] + (1.0 - beta_two) * grad * grad
            step = (new_first * scale_one) / (jnp.sqrt(new_second * scale_two) + adam_eps) + decay_rate * weight
            first[rows, cols] = new_first
            second[rows, cols] = new_second
            update[rows, cols] = step
            row_update += step * step
            row_weight += weight * weight
        tensor = ids[rows, :]
        return tuple(
            (
                sums[t][0] + jnp.where(tensor == t, row_update, 0.0),
                sums[t][1] + jnp.where(tensor == t, row_weight, 0.0),
            )
            for t in range(LAYERS)
        )

    zero = jnp.zeros((GROUP, LANES), jnp.float32)
    sums = lax.fori_loop(0, blocks, compute, tuple((zero, zero) for _ in range(LAYERS)))

    lane_id = lax.broadcasted_iota(jnp.int32, (1, LANES), 1)
    packed = jnp.zeros((1, LANES), jnp.float32)
    for t in range(LAYERS):
        for part in range(2):
            packed = jnp.where(lane_id == t + LAYERS * part, jnp.sum(sums[t][part]), packed)
    partial[...] = jnp.broadcast_to(packed, (GROUP, LANES))

    for other in others:
        pltpu.make_async_remote_copy(
            src_ref=partial.at[pl.ds(0, 1)],
            dst_ref=totals.at[pl.ds(me, 1)],
            send_sem=total_send_sem,
            recv_sem=total_recv_sem,
            device_id=other,
            device_id_type=LOGICAL,
        ).start()
    pltpu.make_async_copy(partial.at[pl.ds(0, 1)], totals.at[pl.ds(me, 1)], total_recv_sem).start()
    pltpu.make_async_copy(partial.at[pl.ds(0, 1)], spare.at[0, pl.ds(1, 1), pl.ds(0, LANES)], total_send_sem).start()
    pltpu.make_async_copy(totals, totals, total_recv_sem).wait()
    summed = jnp.sum(totals[...], axis=0, keepdims=True)
    ratio = jnp.sqrt(pltpu.roll(summed, LANES - LAYERS, 1)) / (jnp.sqrt(summed) + trust_eps)
    hot = lax.broadcasted_iota(jnp.int32, (devices, LANES), 1) == ids[...]
    per_row = jnp.sum(jnp.where(hot, ratio, 0.0), axis=1, keepdims=True)
    row_ratio[...] = jnp.broadcast_to(per_row, (devices, LANES))

    pltpu.make_async_copy(sending, source, send_sem).wait()
    pltpu.make_async_copy(totals, totals, total_send_sem).wait()


def finish_kernel(weights, update, first, second, row_ratio, new_master, new_one, new_two, fresh, sem_one, sem_two, sem_fresh):
    rows, width = weights.shape
    chunk = 32
    writes = []
    for index in range(rows // chunk):
        at = pl.ds(index * chunk, chunk)
        writes.append(pltpu.make_async_copy(first.at[at], new_one.at[at], sem_one.at[index]))
        writes.append(pltpu.make_async_copy(second.at[at], new_two.at[at], sem_two.at[index]))
    for write in writes:
        write.start()
    for index in range(rows // chunk):
        at = pl.ds(index * chunk, chunk)
        scale = learn_rate * row_ratio[at, :]
        for lane in range(0, width, LANES):
            cols = pl.ds(lane, LANES)
            fresh[at, cols] = weights[at, cols] - scale * update[at, cols]
        writes.append(pltpu.make_async_copy(fresh.at[at], new_master.at[at], sem_fresh.at[index]))
        writes[-1].start()
    for write in writes:
        write.wait()


def local(master, moment_one, moment_two, gradient, partner, tensor_of_row):
    rows_dev, width = master.shape
    devices = partner.shape[0]
    operands = (
        partner.reshape(1, devices), tensor_of_row.reshape(devices, devices), master, moment_one, moment_two, gradient
    )
    operands = [pltpu.with_memory_space_constraint(operand, pltpu.HBM) for operand in operands]
    vmem = pl.BlockSpec(memory_space=pltpu.VMEM)
    hbm = pl.BlockSpec(memory_space=pltpu.HBM)
    block = pltpu.VMEM((rows_dev, width), jnp.float32)
    stack = pltpu.VMEM((3, rows_dev, width), jnp.float32)
    dma = pltpu.SemaphoreType.DMA
    weights, update, first, second, row_ratio = pl.pallas_call(
        exchange_kernel,
        out_shape=(block, block, block, block, pltpu.VMEM((rows_dev, LANES), jnp.float32)),
        in_specs=[hbm] * 6,
        out_specs=(vmem,) * 5,
        scratch_shapes=[
            stack,
            stack,
            pltpu.VMEM((3, GROUP, width), jnp.float32),
            pltpu.VMEM((devices, devices), jnp.int32),
            pltpu.VMEM((rows_dev, LANES), jnp.int32),
            pltpu.VMEM((1, devices), jnp.int32),
            pltpu.VMEM((GROUP, devices), jnp.int32),
            pltpu.SMEM((1, devices), jnp.int32),
            pltpu.VMEM((GROUP, LANES), jnp.float32),
            pltpu.VMEM((devices, LANES), jnp.float32),
            dma((3,)),
            dma,
            dma,
            dma,
            dma,
            dma((devices // GROUP,)),
            dma,
            dma,
        ],
        compiler_params=pltpu.CompilerParams(
            collective_id=0, has_side_effects=True, vmem_limit_bytes=24 * 1024 * 1024
        ),
        name="exchange",
    )(*operands)
    whole = jax.ShapeDtypeStruct((rows_dev, width), jnp.float32)
    return pl.pallas_call(
        finish_kernel,
        out_shape=(whole,) * 3,
        in_specs=[vmem] * 5,
        out_specs=(hbm,) * 3,
        scratch_shapes=[block, dma((4,)), dma((4,)), dma((4,))],
        compiler_params=pltpu.CompilerParams(vmem_limit_bytes=8 * 1024 * 1024),
        name="finish",
    )(weights, update, first, second, row_ratio)


def solution(mesh):
    finer = Mesh(mesh.devices.reshape(4, 2, 4, 2, 2), AXES)
    in_specs = (P(AXES, None), P(AXES, None), P(AXES, None), P(AXES, None), P(), P())
    out_specs = (P(AXES, None), P(AXES, None), P(AXES, None))
    return jax.shard_map(local, mesh=finer, in_specs=in_specs, out_specs=out_specs, check_vma=False)
```

```python
import functools

import jax
import jax.numpy as jnp
from jax import lax
from jax.experimental import pallas as pl
from jax.experimental.pallas import tpu as pltpu
from jax.sharding import Mesh
from jax.sharding import PartitionSpec as P

LAYERS = 8
AXES = ("grp_0", "grp_1", "grp_2", "sub_0", "sub_1")
LOGICAL = pl.DeviceIdType.LOGICAL
STRIDE = 37
LANES = 128
GROUP = 8
BLOCK_ORDER = (
    (2, 0, 0), (2, 0, 1), (2, 1, 0), (2, 1, 1), (1, 1, 1), (3, 1, 1), (1, 0, 1), (1, 1, 0),
    (3, 0, 1), (3, 1, 0), (0, 1, 1), (1, 0, 0), (3, 0, 0), (0, 0, 1), (0, 1, 0), (0, 0, 0),
)


beta_one = 0.9
beta_two = 0.999
step_count = 10
adam_eps = 1e-06
trust_eps = 1e-06
learn_rate = 0.05
decay_rate = 0.01


def own_place():
    y = lax.axis_index("grp_0")
    z = lax.axis_index("grp_1") * 2 + lax.axis_index("sub_0")
    x = lax.axis_index("grp_2")
    core = lax.axis_index("sub_1")
    return x, y, z, core


def number_of(x, y, z, core):
    return (((y * 2 + z // 2) * 4 + x) * 2 + z % 2) * 2 + core


def exchange_kernel(
    partner, tensor_of_row, master, moment_one, moment_two, gradient,
    weights, update, first, second, row_ratio,
    source, sending, spare, row_tensor, ids, partner_row, inverse_row, inverse, partial, totals,
    load_sem, partner_sem, tensor_sem, grad_sem, send_sem, recv_sem, total_send_sem, total_recv_sem,
):
    devices, width = weights.shape
    blocks = devices // GROUP
    x, y, z, core = own_place()
    me = number_of(x, y, z, core)
    arrived = (weights, first, second)

    turn = 1 - 2 * core

    def spread(step):
        offset = (step * STRIDE) % devices
        return sum(d * (4 - d) for d in (offset // 32, offset // 8 % 4, offset // 2 % 4))

    def target(step):
        offset = (step * STRIDE) % devices
        return number_of(
            (x + turn * (offset // 32) + 4) % 4,
            (y + turn * (offset // 8 % 4) + 4) % 4,
            (z + turn * (offset // 2 % 4) + 4) % 4,
            (core + offset % 2) % 2,
        )

    x_part = [((x + d) % 4) * 4 for d in range(4)]
    y_part = [((y + d) % 4) * 32 for d in range(4)]
    z_part = [((z + d) % 4) // 2 * 16 + ((z + d) % 4) % 2 * 2 for d in range(4)]
    core_part = [(core + d) % 2 for d in range(2)]
    places = [(dx, dy, dz, dc) for dx in range(4) for dy in range(4) for dz in range(4) for dc in range(2)]
    places.remove((0, 0, 0, 0))
    places.sort(key=lambda d: sum(min(v, 4 - v) for v in d[:3]), reverse=True)
    others = [x_part[dx] + y_part[dy] + z_part[dz] + core_part[dc] for dx, dy, dz, dc in places]

    partner_load = pltpu.make_async_copy(partner, partner_row, partner_sem)
    partner_load.start()
    loads = [
        pltpu.make_async_copy(array, source.at[k], load_sem.at[k])
        for k, array in enumerate((master, moment_one, moment_two))
    ]
    for load in loads:
        load.start()
    grad_load = pltpu.make_async_copy(gradient, update, grad_sem)
    grad_load.start()
    tensor_load = pltpu.make_async_copy(tensor_of_row, row_tensor, tensor_sem)
    tensor_load.start()

    barrier = pltpu.get_barrier_semaphore()

    for other in others:
        pl.semaphore_signal(barrier, inc=1, device_id=other, device_id_type=LOGICAL)

    down = lax.broadcasted_iota(jnp.int32, (devices, devices), 0)
    across = lax.broadcasted_iota(jnp.int32, (devices, devices), 1)
    partner_load.wait()
    holder = jnp.broadcast_to(partner_row[...], (devices, devices))
    rank_of = jnp.sum(jnp.where(holder == down, across, 0), axis=1, keepdims=True)
    turned = jnp.sum(jnp.where(down == across, rank_of, 0), axis=0, keepdims=True)
    inverse_row[...] = jnp.broadcast_to(turned, (GROUP, devices))
    inverse_move = pltpu.make_async_copy(inverse_row.at[pl.ds(0, 1)], inverse, partner_sem)
    inverse_move.start()
    tensor_load.wait()
    mine = jnp.where(holder == me, row_tensor[...], 0)
    ids[...] = jnp.broadcast_to(jnp.sum(mine, axis=1, keepdims=True), (devices, LANES))
    inverse_move.wait()

    for load in loads:
        load.wait()

    def pick(step):
        row = inverse[0, target(step)] & (devices - 1)
        for k in range(3):
            sending[k, pl.ds(step, 1), :] = source[k, pl.ds(row, 1), :]

    def send(step):
        there = target(step)
        for k in range(3):
            pltpu.make_async_remote_copy(
                src_ref=sending.at[k, pl.ds(step, 1)],
                dst_ref=arrived[k].at[pl.ds(me, 1)],
                send_sem=send_sem,
                recv_sem=recv_sem.at[me // GROUP],
                device_id=there,
                device_id_type=LOGICAL,
            ).start()


    def keep():
        for k in range(3):
            pltpu.make_async_copy(
                sending.at[k, pl.ds(0, 1)], arrived[k].at[pl.ds(me, 1)], recv_sem.at[me // GROUP]
            ).start()
            pltpu.make_async_copy(sending.at[k, pl.ds(0, 1)], spare.at[k, pl.ds(0, 1)], send_sem).start()

    def pick_group(group):
        for j in range(GROUP):
            pick(group * GROUP + j)

    pick_group(0)
    pick_group(1)
    pl.semaphore_wait(barrier, devices - 1)
    keep()
    for step in range(1, GROUP):
        if spread(step) > 3:
            send(step)

    def send_far(step):
        @pl.when(spread(step) > 3)
        def _():
            send(step)

    def round_of(group, carry):
        pick_group(group + 1)
        for j in range(GROUP):
            send_far(group * GROUP + j)
        return carry

    lax.fori_loop(1, blocks - 1, round_of, 0)
    for step in range((blocks - 1) * GROUP, devices):
        if spread(step) > 3:
            send(step)
    for step in range(1, devices):
        if spread(step) <= 3:
            send(step)

    grad_load.wait()
    scale_one = 1.0 / (1.0 - beta_one**step_count)
    scale_two = 1.0 / (1.0 - beta_two**step_count)

    def compute(_, carry):
        y_code, z_code, x_code, sums = carry
        block = ((y + y_code % 4) % 4 * 2 + (z // 2 + z_code % 2) % 2) * 2 + (x // 2 + x_code % 2) % 2
        pltpu.make_async_copy(
            sending.at[0, pl.ds(0, 3 * GROUP)], source.at[0, pl.ds(0, 3 * GROUP)], recv_sem.at[block]
        ).wait()
        rows = pl.ds(pl.multiple_of(block * GROUP, GROUP), GROUP)
        row_update = jnp.zeros((GROUP, LANES), jnp.float32)
        row_weight = jnp.zeros((GROUP, LANES), jnp.float32)
        for lane in range(0, width, LANES):
            cols = pl.ds(lane, LANES)
            grad = update[rows, cols]
            weight = weights[rows, cols]
            new_first = beta_one * first[rows, cols] + (1.0 - beta_one) * grad
            new_second = beta_two * second[rows, cols] + (1.0 - beta_two) * grad * grad
            step = (new_first * scale_one) / (jnp.sqrt(new_second * scale_two) + adam_eps) + decay_rate * weight
            first[rows, cols] = new_first
            second[rows, cols] = new_second
            update[rows, cols] = step
            row_update += step * step
            row_weight += weight * weight
        tensor = ids[rows, :]
        sums = tuple(
            (
                sums[t][0] + jnp.where(tensor == t, row_update, 0.0),
                sums[t][1] + jnp.where(tensor == t, row_weight, 0.0),
            )
            for t in range(LAYERS)
        )
        return y_code // 4, z_code // 2, x_code // 2, sums

    zero = jnp.zeros((GROUP, LANES), jnp.float32)
    codes = [sum(d[i] * base**k for k, d in enumerate(BLOCK_ORDER)) for i, base in enumerate((4, 2, 2))]
    carry = (*[jnp.int32(code) for code in codes], tuple((zero, zero) for _ in range(LAYERS)))
    sums = lax.fori_loop(0, blocks, compute, carry)[3]

    lane_id = lax.broadcasted_iota(jnp.int32, (1, LANES), 1)
    packed = jnp.zeros((1, LANES), jnp.float32)
    for t in range(LAYERS):
        for part in range(2):
            packed = jnp.where(lane_id == t + LAYERS * part, jnp.sum(sums[t][part]), packed)
    partial[...] = jnp.broadcast_to(packed, (GROUP, LANES))

    for other in others:
        pltpu.make_async_remote_copy(
            src_ref=partial.at[pl.ds(0, 1)],
            dst_ref=totals.at[pl.ds(me, 1)],
            send_sem=total_send_sem,
            recv_sem=total_recv_sem,
            device_id=other,
            device_id_type=LOGICAL,
        ).start()
    pltpu.make_async_copy(partial.at[pl.ds(0, 1)], totals.at[pl.ds(me, 1)], total_recv_sem).start()
    pltpu.make_async_copy(partial.at[pl.ds(0, 1)], spare.at[0, pl.ds(1, 1), pl.ds(0, LANES)], total_send_sem).start()
    pltpu.make_async_copy(totals, totals, total_recv_sem).wait()
    summed = jnp.sum(totals[...], axis=0, keepdims=True)
    ratio = jnp.sqrt(pltpu.roll(summed, LANES - LAYERS, 1)) / (jnp.sqrt(summed) + trust_eps)
    hot = lax.broadcasted_iota(jnp.int32, (devices, LANES), 1) == ids[...]
    per_row = jnp.sum(jnp.where(hot, ratio, 0.0), axis=1, keepdims=True)
    row_ratio[...] = jnp.broadcast_to(per_row, (devices, LANES))

    pltpu.make_async_copy(sending, source, send_sem).wait()
    pltpu.make_async_copy(totals, totals, total_send_sem).wait()


def finish_kernel(weights, update, first, second, row_ratio, new_master, new_one, new_two, fresh, sem_one, sem_two, sem_fresh):
    rows, width = weights.shape
    chunk = 32
    writes = []
    for index in range(rows // chunk):
        at = pl.ds(index * chunk, chunk)
        writes.append(pltpu.make_async_copy(first.at[at], new_one.at[at], sem_one.at[index]))
        writes.append(pltpu.make_async_copy(second.at[at], new_two.at[at], sem_two.at[index]))
    for write in writes:
        write.start()
    for index in range(rows // chunk):
        at = pl.ds(index * chunk, chunk)
        scale = learn_rate * row_ratio[at, :]
        for lane in range(0, width, LANES):
            cols = pl.ds(lane, LANES)
            fresh[at, cols] = weights[at, cols] - scale * update[at, cols]
        writes.append(pltpu.make_async_copy(fresh.at[at], new_master.at[at], sem_fresh.at[index]))
        writes[-1].start()
    for write in writes:
        write.wait()


def local(master, moment_one, moment_two, gradient, partner, tensor_of_row):
    rows_dev, width = master.shape
    devices = partner.shape[0]
    operands = (
        partner.reshape(1, devices), tensor_of_row.reshape(devices, devices), master, moment_one, moment_two, gradient
    )
    operands = [pltpu.with_memory_space_constraint(operand, pltpu.HBM) for operand in operands]
    vmem = pl.BlockSpec(memory_space=pltpu.VMEM)
    hbm = pl.BlockSpec(memory_space=pltpu.HBM)
    block = pltpu.VMEM((rows_dev, width), jnp.float32)
    stack = pltpu.VMEM((3, rows_dev, width), jnp.float32)
    dma = pltpu.SemaphoreType.DMA
    weights, update, first, second, row_ratio = pl.pallas_call(
        exchange_kernel,
        out_shape=(block, block, block, block, pltpu.VMEM((rows_dev, LANES), jnp.float32)),
        in_specs=[hbm] * 6,
        out_specs=(vmem,) * 5,
        scratch_shapes=[
            stack,
            stack,
            pltpu.VMEM((3, GROUP, width), jnp.float32),
            pltpu.VMEM((devices, devices), jnp.int32),
            pltpu.VMEM((rows_dev, LANES), jnp.int32),
            pltpu.VMEM((1, devices), jnp.int32),
            pltpu.VMEM((GROUP, devices), jnp.int32),
            pltpu.SMEM((1, devices), jnp.int32),
            pltpu.VMEM((GROUP, LANES), jnp.float32),
            pltpu.VMEM((devices, LANES), jnp.float32),
            dma((3,)),
            dma,
            dma,
            dma,
            dma,
            dma((devices // GROUP,)),
            dma,
            dma,
        ],
        compiler_params=pltpu.CompilerParams(
            collective_id=0, has_side_effects=True, vmem_limit_bytes=24 * 1024 * 1024
        ),
        name="exchange",
    )(*operands)
    whole = jax.ShapeDtypeStruct((rows_dev, width), jnp.float32)
    return pl.pallas_call(
        finish_kernel,
        out_shape=(whole,) * 3,
        in_specs=[vmem] * 5,
        out_specs=(hbm,) * 3,
        scratch_shapes=[block, dma((4,)), dma((4,)), dma((4,))],
        compiler_params=pltpu.CompilerParams(vmem_limit_bytes=8 * 1024 * 1024),
        name="finish",
    )(weights, update, first, second, row_ratio)


def solution(mesh):
    finer = Mesh(mesh.devices.reshape(4, 2, 4, 2, 2), AXES)
    in_specs = (P(AXES, None), P(AXES, None), P(AXES, None), P(AXES, None), P(), P())
    out_specs = (P(AXES, None), P(AXES, None), P(AXES, None))
    return jax.shard_map(local, mesh=finer, in_specs=in_specs, out_specs=out_specs, check_vma=False)
```

```python
import functools

import jax
import jax.numpy as jnp
from jax import lax
from jax.experimental import pallas as pl
from jax.experimental.pallas import tpu as pltpu
from jax.sharding import Mesh
from jax.sharding import PartitionSpec as P

LAYERS = 8
AXES = ("grp_0", "grp_1", "grp_2", "sub_0", "sub_1")
LOGICAL = pl.DeviceIdType.LOGICAL
STRIDE = 19
LANES = 128
GROUP = 8
BLOCK_ORDER = (
    (2, 0, 0), (2, 0, 1), (2, 1, 0), (2, 1, 1), (1, 1, 1), (3, 1, 1), (1, 0, 1), (1, 1, 0),
    (3, 0, 1), (3, 1, 0), (0, 1, 1), (1, 0, 0), (3, 0, 0), (0, 0, 1), (0, 1, 0), (0, 0, 0),
)


beta_one = 0.9
beta_two = 0.999
step_count = 10
adam_eps = 1e-06
trust_eps = 1e-06
learn_rate = 0.05
decay_rate = 0.01


def own_place():
    y = lax.axis_index("grp_0")
    z = lax.axis_index("grp_1") * 2 + lax.axis_index("sub_0")
    x = lax.axis_index("grp_2")
    core = lax.axis_index("sub_1")
    return x, y, z, core


def number_of(x, y, z, core):
    return (((y * 2 + z // 2) * 4 + x) * 2 + z % 2) * 2 + core


def exchange_kernel(
    partner, tensor_of_row, master, moment_one, moment_two, gradient,
    weights, update, first, second, row_ratio,
    source, sending, spare, row_tensor, ids, partner_row, inverse_row, inverse, partial, totals,
    load_sem, partner_sem, tensor_sem, grad_sem, send_sem, recv_sem, total_send_sem, total_recv_sem,
):
    devices, width = weights.shape
    blocks = devices // GROUP
    x, y, z, core = own_place()
    me = number_of(x, y, z, core)
    arrived = (weights, first, second)

    turn = 1 - 2 * core

    def spread(step):
        offset = (step * STRIDE) % devices
        return sum(d * (4 - d) for d in (offset // 16 % 4, offset // 4 % 4, offset // 1 % 4))

    def target(step):
        offset = (step * STRIDE) % devices
        return number_of(
            (x + turn * (offset // 16 % 4) + 4) % 4,
            (y + turn * (offset // 4 % 4) + 4) % 4,
            (z + turn * (offset // 1 % 4) + 4) % 4,
            (core + offset // 64 % 2) % 2,
        )

    x_part = [((x + d) % 4) * 4 for d in range(4)]
    y_part = [((y + d) % 4) * 32 for d in range(4)]
    z_part = [((z + d) % 4) // 2 * 16 + ((z + d) % 4) % 2 * 2 for d in range(4)]
    core_part = [(core + d) % 2 for d in range(2)]
    places = [(dx, dy, dz, dc) for dx in range(4) for dy in range(4) for dz in range(4) for dc in range(2)]
    places.remove((0, 0, 0, 0))
    places.sort(key=lambda d: sum(min(v, 4 - v) for v in d[:3]), reverse=True)
    others = [x_part[dx] + y_part[dy] + z_part[dz] + core_part[dc] for dx, dy, dz, dc in places]

    partner_load = pltpu.make_async_copy(partner, partner_row, partner_sem)
    partner_load.start()
    loads = [
        pltpu.make_async_copy(array, source.at[k], load_sem.at[k])
        for k, array in enumerate((master, moment_one, moment_two))
    ]
    for load in loads:
        load.start()
    grad_load = pltpu.make_async_copy(gradient, update, grad_sem)
    grad_load.start()
    tensor_load = pltpu.make_async_copy(tensor_of_row, row_tensor, tensor_sem)
    tensor_load.start()

    barrier = pltpu.get_barrier_semaphore()

    for other in others:
        pl.semaphore_signal(barrier, inc=1, device_id=other, device_id_type=LOGICAL)

    down = lax.broadcasted_iota(jnp.int32, (devices, devices), 0)
    across = lax.broadcasted_iota(jnp.int32, (devices, devices), 1)
    partner_load.wait()
    holder = jnp.broadcast_to(partner_row[...], (devices, devices))
    rank_of = jnp.sum(jnp.where(holder == down, across, 0), axis=1, keepdims=True)
    turned = jnp.sum(jnp.where(down == across, rank_of, 0), axis=0, keepdims=True)
    inverse_row[...] = jnp.broadcast_to(turned, (GROUP, devices))
    inverse_move = pltpu.make_async_copy(inverse_row.at[pl.ds(0, 1)], inverse, partner_sem)
    inverse_move.start()
    tensor_load.wait()
    mine = jnp.where(holder == me, row_tensor[...], 0)
    ids[...] = jnp.broadcast_to(jnp.sum(mine, axis=1, keepdims=True), (devices, LANES))
    inverse_move.wait()

    for load in loads:
        load.wait()

    def pick(step):
        row = inverse[0, target(step)] & (devices - 1)
        for k in range(3):
            sending[k, pl.ds(step, 1), :] = source[k, pl.ds(row, 1), :]

    def send(step):
        there = target(step)
        for k in range(3):
            pltpu.make_async_remote_copy(
                src_ref=sending.at[k, pl.ds(step, 1)],
                dst_ref=arrived[k].at[pl.ds(me, 1)],
                send_sem=send_sem,
                recv_sem=recv_sem.at[me // GROUP],
                device_id=there,
                device_id_type=LOGICAL,
            ).start()


    def keep():
        for k in range(3):
            pltpu.make_async_copy(
                sending.at[k, pl.ds(0, 1)], arrived[k].at[pl.ds(me, 1)], recv_sem.at[me // GROUP]
            ).start()
            pltpu.make_async_copy(sending.at[k, pl.ds(0, 1)], spare.at[k, pl.ds(0, 1)], send_sem).start()

    def pick_group(group):
        for j in range(GROUP):
            pick(group * GROUP + j)

    pick_group(0)
    pick_group(1)
    pl.semaphore_wait(barrier, devices - 1)
    keep()
    for step in range(1, GROUP):
        if spread(step) > 3:
            send(step)

    def send_far(step):
        @pl.when(spread(step) > 3)
        def _():
            send(step)

    def round_of(group, carry):
        pick_group(group + 1)
        for j in range(GROUP):
            send_far(group * GROUP + j)
        return carry

    lax.fori_loop(1, blocks - 1, round_of, 0)
    for step in range((blocks - 1) * GROUP, devices):
        if spread(step) > 3:
            send(step)
    for step in range(1, devices):
        if spread(step) <= 3:
            send(step)

    grad_load.wait()
    scale_one = 1.0 / (1.0 - beta_one**step_count)
    scale_two = 1.0 / (1.0 - beta_two**step_count)

    def compute(_, carry):
        y_code, z_code, x_code, sums = carry
        block = ((y + y_code % 4) % 4 * 2 + (z // 2 + z_code % 2) % 2) * 2 + (x // 2 + x_code % 2) % 2
        pltpu.make_async_copy(
            sending.at[0, pl.ds(0, 3 * GROUP)], source.at[0, pl.ds(0, 3 * GROUP)], recv_sem.at[block]
        ).wait()
        rows = pl.ds(pl.multiple_of(block * GROUP, GROUP), GROUP)
        row_update = jnp.zeros((GROUP, LANES), jnp.float32)
        row_weight = jnp.zeros((GROUP, LANES), jnp.float32)
        for lane in range(0, width, LANES):
            cols = pl.ds(lane, LANES)
            grad = update[rows, cols]
            weight = weights[rows, cols]
            new_first = beta_one * first[rows, cols] + (1.0 - beta_one) * grad
            new_second = beta_two * second[rows, cols] + (1.0 - beta_two) * grad * grad
            step = (new_first * scale_one) / (jnp.sqrt(new_second * scale_two) + adam_eps) + decay_rate * weight
            first[rows, cols] = new_first
            second[rows, cols] = new_second
            update[rows, cols] = step
            row_update += step * step
            row_weight += weight * weight
        tensor = ids[rows, :]
        sums = tuple(
            (
                sums[t][0] + jnp.where(tensor == t, row_update, 0.0),
                sums[t][1] + jnp.where(tensor == t, row_weight, 0.0),
            )
            for t in range(LAYERS)
        )
        return y_code // 4, z_code // 2, x_code // 2, sums

    zero = jnp.zeros((GROUP, LANES), jnp.float32)
    codes = [sum(d[i] * base**k for k, d in enumerate(BLOCK_ORDER)) for i, base in enumerate((4, 2, 2))]
    carry = (*[jnp.int32(code) for code in codes], tuple((zero, zero) for _ in range(LAYERS)))
    sums = lax.fori_loop(0, blocks, compute, carry)[3]

    kinds = 2 * LAYERS
    kind_id = lax.broadcasted_iota(jnp.int32, (kinds, LANES), 0)
    lane_id = lax.broadcasted_iota(jnp.int32, (kinds, LANES), 1)
    stacked = jnp.zeros((kinds, LANES), jnp.float32)
    for t in range(LAYERS):
        for part in range(2):
            folded = jnp.sum(sums[t][part], axis=0, keepdims=True)
            stacked = jnp.where(kind_id == t + LAYERS * part, folded, stacked)
    column = jnp.sum(stacked, axis=1, keepdims=True)
    packed = jnp.sum(jnp.where(kind_id == lane_id, column, 0.0), axis=0, keepdims=True)
    partial[...] = jnp.broadcast_to(packed, (GROUP, LANES))

    for other in others:
        pltpu.make_async_remote_copy(
            src_ref=partial.at[pl.ds(0, 1)],
            dst_ref=totals.at[pl.ds(me, 1)],
            send_sem=total_send_sem,
            recv_sem=total_recv_sem,
            device_id=other,
            device_id_type=LOGICAL,
        ).start()
    pltpu.make_async_copy(partial.at[pl.ds(0, 1)], totals.at[pl.ds(me, 1)], total_recv_sem).start()
    pltpu.make_async_copy(partial.at[pl.ds(0, 1)], spare.at[0, pl.ds(1, 1), pl.ds(0, LANES)], total_send_sem).start()
    pltpu.make_async_copy(totals, totals, total_recv_sem).wait()
    summed = jnp.sum(totals[...], axis=0, keepdims=True)
    ratio = jnp.sqrt(pltpu.roll(summed, LANES - LAYERS, 1)) / (jnp.sqrt(summed) + trust_eps)
    hot = lax.broadcasted_iota(jnp.int32, (devices, LANES), 1) == ids[...]
    per_row = jnp.sum(jnp.where(hot, ratio, 0.0), axis=1, keepdims=True)
    row_ratio[...] = jnp.broadcast_to(per_row, (devices, LANES))

    pltpu.make_async_copy(sending, source, send_sem).wait()
    pltpu.make_async_copy(totals, totals, total_send_sem).wait()


def finish_kernel(weights, update, first, second, row_ratio, new_master, new_one, new_two, fresh, sem_one, sem_two, sem_fresh):
    rows, width = weights.shape
    chunk = 32
    writes = []
    for index in range(rows // chunk):
        at = pl.ds(index * chunk, chunk)
        writes.append(pltpu.make_async_copy(first.at[at], new_one.at[at], sem_one.at[index]))
        writes.append(pltpu.make_async_copy(second.at[at], new_two.at[at], sem_two.at[index]))
    for write in writes:
        write.start()
    for index in range(rows // chunk):
        at = pl.ds(index * chunk, chunk)
        scale = learn_rate * row_ratio[at, :]
        for lane in range(0, width, LANES):
            cols = pl.ds(lane, LANES)
            fresh[at, cols] = weights[at, cols] - scale * update[at, cols]
        writes.append(pltpu.make_async_copy(fresh.at[at], new_master.at[at], sem_fresh.at[index]))
        writes[-1].start()
    for write in writes:
        write.wait()


def local(master, moment_one, moment_two, gradient, partner, tensor_of_row):
    rows_dev, width = master.shape
    devices = partner.shape[0]
    operands = (
        partner.reshape(1, devices), tensor_of_row.reshape(devices, devices), master, moment_one, moment_two, gradient
    )
    operands = [pltpu.with_memory_space_constraint(operand, pltpu.HBM) for operand in operands]
    vmem = pl.BlockSpec(memory_space=pltpu.VMEM)
    hbm = pl.BlockSpec(memory_space=pltpu.HBM)
    block = pltpu.VMEM((rows_dev, width), jnp.float32)
    stack = pltpu.VMEM((3, rows_dev, width), jnp.float32)
    dma = pltpu.SemaphoreType.DMA
    weights, update, first, second, row_ratio = pl.pallas_call(
        exchange_kernel,
        out_shape=(block, block, block, block, pltpu.VMEM((rows_dev, LANES), jnp.float32)),
        in_specs=[hbm] * 6,
        out_specs=(vmem,) * 5,
        scratch_shapes=[
            stack,
            stack,
            pltpu.VMEM((3, GROUP, width), jnp.float32),
            pltpu.VMEM((devices, devices), jnp.int32),
            pltpu.VMEM((rows_dev, LANES), jnp.int32),
            pltpu.VMEM((1, devices), jnp.int32),
            pltpu.VMEM((GROUP, devices), jnp.int32),
            pltpu.SMEM((1, devices), jnp.int32),
            pltpu.VMEM((GROUP, LANES), jnp.float32),
            pltpu.VMEM((devices, LANES), jnp.float32),
            dma((3,)),
            dma,
            dma,
            dma,
            dma,
            dma((devices // GROUP,)),
            dma,
            dma,
        ],
        compiler_params=pltpu.CompilerParams(
            collective_id=0, has_side_effects=True, vmem_limit_bytes=24 * 1024 * 1024
        ),
        name="exchange",
    )(*operands)
    whole = jax.ShapeDtypeStruct((rows_dev, width), jnp.float32)
    return pl.pallas_call(
        finish_kernel,
        out_shape=(whole,) * 3,
        in_specs=[vmem] * 5,
        out_specs=(hbm,) * 3,
        scratch_shapes=[block, dma((4,)), dma((4,)), dma((4,))],
        compiler_params=pltpu.CompilerParams(vmem_limit_bytes=8 * 1024 * 1024),
        name="finish",
    )(weights, update, first, second, row_ratio)


def solution(mesh):
    finer = Mesh(mesh.devices.reshape(4, 2, 4, 2, 2), AXES)
    in_specs = (P(AXES, None), P(AXES, None), P(AXES, None), P(AXES, None), P(), P())
    out_specs = (P(AXES, None), P(AXES, None), P(AXES, None))
    return jax.shard_map(local, mesh=finer, in_specs=in_specs, out_specs=out_specs, check_vma=False)
```

```python
import functools

import jax
import jax.numpy as jnp
from jax import lax
from jax.experimental import pallas as pl
from jax.experimental.pallas import tpu as pltpu
from jax.sharding import Mesh
from jax.sharding import PartitionSpec as P

LAYERS = 8
AXES = ("grp_0", "grp_1", "grp_2", "sub_0", "sub_1")
LOGICAL = pl.DeviceIdType.LOGICAL
STRIDE = 19
LANES = 128
GROUP = 8
BLOCK_ORDER = (
    (2, 0, 0), (0, 1, 1), (1, 1, 0), (3, 1, 0), (1, 1, 1), (3, 1, 1), (2, 1, 0), (1, 0, 1),
    (3, 0, 1), (2, 0, 1), (2, 1, 1), (0, 1, 0), (1, 0, 0), (3, 0, 0), (0, 0, 1), (0, 0, 0),
)


beta_one = 0.9
beta_two = 0.999
step_count = 10
adam_eps = 1e-06
trust_eps = 1e-06
learn_rate = 0.05
decay_rate = 0.01


def own_place():
    y = lax.axis_index("grp_0")
    z = lax.axis_index("grp_1") * 2 + lax.axis_index("sub_0")
    x = lax.axis_index("grp_2")
    core = lax.axis_index("sub_1")
    return x, y, z, core


def number_of(x, y, z, core):
    return (((y * 2 + z // 2) * 4 + x) * 2 + z % 2) * 2 + core


def exchange_kernel(
    partner, tensor_of_row, master, moment_one, moment_two, gradient,
    weights, update, first, second, row_ratio,
    source, sending, spare, row_tensor, ids, partner_row, inverse_row, inverse, partial, totals,
    load_sem, partner_sem, tensor_sem, grad_sem, send_sem, recv_sem, total_send_sem, total_recv_sem,
):
    devices, width = weights.shape
    blocks = devices // GROUP
    x, y, z, core = own_place()
    me = number_of(x, y, z, core)
    arrived = (weights, first, second)

    turn = 1 - 2 * core

    def spread(step):
        offset = (step * STRIDE) % devices
        return sum(d * (4 - d) for d in (offset // 16 % 4, offset // 4 % 4, offset // 1 % 4))

    def target(step):
        offset = (step * STRIDE) % devices
        return number_of(
            (x + turn * (offset // 16 % 4) + 4) % 4,
            (y + turn * (offset // 4 % 4) + 4) % 4,
            (z + turn * (offset // 1 % 4) + 4) % 4,
            (core + offset // 64 % 2) % 2,
        )

    x_part = [((x + d) % 4) * 4 for d in range(4)]
    y_part = [((y + d) % 4) * 32 for d in range(4)]
    z_part = [((z + d) % 4) // 2 * 16 + ((z + d) % 4) % 2 * 2 for d in range(4)]
    core_part = [(core + d) % 2 for d in range(2)]
    places = [(dx, dy, dz, dc) for dx in range(4) for dy in range(4) for dz in range(4) for dc in range(2)]
    places.remove((0, 0, 0, 0))
    places.sort(key=lambda d: sum(min(v, 4 - v) for v in d[:3]), reverse=True)
    others = [x_part[dx] + y_part[dy] + z_part[dz] + core_part[dc] for dx, dy, dz, dc in places]

    partner_load = pltpu.make_async_copy(partner, partner_row, partner_sem)
    partner_load.start()
    loads = [
        pltpu.make_async_copy(array, source.at[k], load_sem.at[k])
        for k, array in enumerate((master, moment_one, moment_two))
    ]
    for load in loads:
        load.start()
    grad_load = pltpu.make_async_copy(gradient, update, grad_sem)
    grad_load.start()
    tensor_load = pltpu.make_async_copy(tensor_of_row, row_tensor, tensor_sem)
    tensor_load.start()

    barrier = pltpu.get_barrier_semaphore()

    for other in others:
        pl.semaphore_signal(barrier, inc=1, device_id=other, device_id_type=LOGICAL)

    down = lax.broadcasted_iota(jnp.int32, (devices, devices), 0)
    across = lax.broadcasted_iota(jnp.int32, (devices, devices), 1)
    partner_load.wait()
    holder = jnp.broadcast_to(partner_row[...], (devices, devices))
    rank_of = jnp.sum(jnp.where(holder == down, across, 0), axis=1, keepdims=True)
    turned = jnp.sum(jnp.where(down == across, rank_of, 0), axis=0, keepdims=True)
    inverse_row[...] = jnp.broadcast_to(turned, (GROUP, devices))
    inverse_move = pltpu.make_async_copy(inverse_row.at[pl.ds(0, 1)], inverse, partner_sem)
    inverse_move.start()
    tensor_load.wait()
    mine = jnp.where(holder == me, row_tensor[...], 0)
    ids[...] = jnp.broadcast_to(jnp.sum(mine, axis=1, keepdims=True), (devices, LANES))
    inverse_move.wait()

    for load in loads:
        load.wait()

    def pick(step):
        row = inverse[0, target(step)] & (devices - 1)
        for k in range(3):
            sending[k, pl.ds(step, 1), :] = source[k, pl.ds(row, 1), :]

    def send(step):
        there = target(step)
        for k in range(3):
            pltpu.make_async_remote_copy(
                src_ref=sending.at[k, pl.ds(step, 1)],
                dst_ref=arrived[k].at[pl.ds(me, 1)],
                send_sem=send_sem,
                recv_sem=recv_sem.at[me // GROUP],
                device_id=there,
                device_id_type=LOGICAL,
            ).start()


    def keep():
        for k in range(3):
            pltpu.make_async_copy(
                sending.at[k, pl.ds(0, 1)], arrived[k].at[pl.ds(me, 1)], recv_sem.at[me // GROUP]
            ).start()
            pltpu.make_async_copy(sending.at[k, pl.ds(0, 1)], spare.at[k, pl.ds(0, 1)], send_sem).start()

    def pick_group(group):
        for j in range(GROUP):
            pick(group * GROUP + j)

    pick_group(0)
    pick_group(1)
    pl.semaphore_wait(barrier, devices - 1)
    keep()
    for step in range(1, GROUP):
        if spread(step) > 3:
            send(step)

    def send_far(step):
        @pl.when(spread(step) > 3)
        def _():
            send(step)

    def round_of(group, carry):
        pick_group(group + 1)
        for j in range(GROUP):
            send_far(group * GROUP + j)
        return carry

    lax.fori_loop(1, blocks - 1, round_of, 0)
    for step in range((blocks - 1) * GROUP, devices):
        if spread(step) > 3:
            send(step)
    for step in range(1, devices):
        if spread(step) <= 3:
            send(step)

    grad_load.wait()
    scale_one = 1.0 / (1.0 - beta_one**step_count)
    scale_two = 1.0 / (1.0 - beta_two**step_count)

    def compute(_, carry):
        y_code, z_code, x_code, sums = carry
        block = ((y + y_code % 4) % 4 * 2 + (z // 2 + z_code % 2) % 2) * 2 + (x // 2 + x_code % 2) % 2
        pltpu.make_async_copy(
            sending.at[0, pl.ds(0, 3 * GROUP)], source.at[0, pl.ds(0, 3 * GROUP)], recv_sem.at[block]
        ).wait()
        rows = pl.ds(pl.multiple_of(block * GROUP, GROUP), GROUP)
        row_update = jnp.zeros((GROUP, LANES), jnp.float32)
        row_weight = jnp.zeros((GROUP, LANES), jnp.float32)
        for lane in range(0, width, LANES):
            cols = pl.ds(lane, LANES)
            grad = update[rows, cols]
            weight = weights[rows, cols]
            new_first = beta_one * first[rows, cols] + (1.0 - beta_one) * grad
            new_second = beta_two * second[rows, cols] + (1.0 - beta_two) * grad * grad
            step = (new_first * scale_one) / (jnp.sqrt(new_second * scale_two) + adam_eps) + decay_rate * weight
            first[rows, cols] = new_first
            second[rows, cols] = new_second
            update[rows, cols] = step
            row_update += step * step
            row_weight += weight * weight
        tensor = ids[rows, :]
        sums = tuple(
            (
                sums[t][0] + jnp.where(tensor == t, row_update, 0.0),
                sums[t][1] + jnp.where(tensor == t, row_weight, 0.0),
            )
            for t in range(LAYERS)
        )
        return y_code // 4, z_code // 2, x_code // 2, sums

    zero = jnp.zeros((GROUP, LANES), jnp.float32)
    codes = [sum(d[i] * base**k for k, d in enumerate(BLOCK_ORDER)) for i, base in enumerate((4, 2, 2))]
    carry = (*[jnp.int32(code) for code in codes], tuple((zero, zero) for _ in range(LAYERS)))
    sums = lax.fori_loop(0, blocks, compute, carry)[3]

    kinds = 2 * LAYERS
    kind_id = lax.broadcasted_iota(jnp.int32, (kinds, LANES), 0)
    lane_id = lax.broadcasted_iota(jnp.int32, (kinds, LANES), 1)
    stacked = jnp.zeros((kinds, LANES), jnp.float32)
    for t in range(LAYERS):
        for part in range(2):
            folded = jnp.sum(sums[t][part], axis=0, keepdims=True)
            stacked = jnp.where(kind_id == t + LAYERS * part, folded, stacked)
    column = jnp.sum(stacked, axis=1, keepdims=True)
    packed = jnp.sum(jnp.where(kind_id == lane_id, column, 0.0), axis=0, keepdims=True)
    partial[...] = jnp.broadcast_to(packed, (GROUP, LANES))

    for other in others:
        pltpu.make_async_remote_copy(
            src_ref=partial.at[pl.ds(0, 1)],
            dst_ref=totals.at[pl.ds(me, 1)],
            send_sem=total_send_sem,
            recv_sem=total_recv_sem,
            device_id=other,
            device_id_type=LOGICAL,
        ).start()
    pltpu.make_async_copy(partial.at[pl.ds(0, 1)], totals.at[pl.ds(me, 1)], total_recv_sem).start()
    pltpu.make_async_copy(partial.at[pl.ds(0, 1)], spare.at[0, pl.ds(1, 1), pl.ds(0, LANES)], total_send_sem).start()
    pltpu.make_async_copy(totals, totals, total_recv_sem).wait()
    summed = jnp.sum(totals[...], axis=0, keepdims=True)
    ratio = jnp.sqrt(pltpu.roll(summed, LANES - LAYERS, 1)) / (jnp.sqrt(summed) + trust_eps)
    hot = lax.broadcasted_iota(jnp.int32, (devices, LANES), 1) == ids[...]
    per_row = jnp.sum(jnp.where(hot, ratio, 0.0), axis=1, keepdims=True)
    row_ratio[...] = jnp.broadcast_to(per_row, (devices, LANES))

    pltpu.make_async_copy(sending, source, send_sem).wait()
    pltpu.make_async_copy(totals, totals, total_send_sem).wait()


def finish_kernel(weights, update, first, second, row_ratio, new_master, new_one, new_two, fresh, sem_one, sem_two, sem_fresh):
    rows, width = weights.shape
    chunk = 32
    writes = []
    for index in range(rows // chunk):
        at = pl.ds(index * chunk, chunk)
        writes.append(pltpu.make_async_copy(first.at[at], new_one.at[at], sem_one.at[index]))
        writes.append(pltpu.make_async_copy(second.at[at], new_two.at[at], sem_two.at[index]))
    for write in writes:
        write.start()
    for index in range(rows // chunk):
        at = pl.ds(index * chunk, chunk)
        scale = learn_rate * row_ratio[at, :]
        for lane in range(0, width, LANES):
            cols = pl.ds(lane, LANES)
            fresh[at, cols] = weights[at, cols] - scale * update[at, cols]
        writes.append(pltpu.make_async_copy(fresh.at[at], new_master.at[at], sem_fresh.at[index]))
        writes[-1].start()
    for write in writes:
        write.wait()


def local(master, moment_one, moment_two, gradient, partner, tensor_of_row):
    rows_dev, width = master.shape
    devices = partner.shape[0]
    operands = (
        partner.reshape(1, devices), tensor_of_row.reshape(devices, devices), master, moment_one, moment_two, gradient
    )
    operands = [pltpu.with_memory_space_constraint(operand, pltpu.HBM) for operand in operands]
    vmem = pl.BlockSpec(memory_space=pltpu.VMEM)
    hbm = pl.BlockSpec(memory_space=pltpu.HBM)
    block = pltpu.VMEM((rows_dev, width), jnp.float32)
    stack = pltpu.VMEM((3, rows_dev, width), jnp.float32)
    dma = pltpu.SemaphoreType.DMA
    weights, update, first, second, row_ratio = pl.pallas_call(
        exchange_kernel,
        out_shape=(block, block, block, block, pltpu.VMEM((rows_dev, LANES), jnp.float32)),
        in_specs=[hbm] * 6,
        out_specs=(vmem,) * 5,
        scratch_shapes=[
            stack,
            stack,
            pltpu.VMEM((3, GROUP, width), jnp.float32),
            pltpu.VMEM((devices, devices), jnp.int32),
            pltpu.VMEM((rows_dev, LANES), jnp.int32),
            pltpu.VMEM((1, devices), jnp.int32),
            pltpu.VMEM((GROUP, devices), jnp.int32),
            pltpu.SMEM((1, devices), jnp.int32),
            pltpu.VMEM((GROUP, LANES), jnp.float32),
            pltpu.VMEM((devices, LANES), jnp.float32),
            dma((3,)),
            dma,
            dma,
            dma,
            dma,
            dma((devices // GROUP,)),
            dma,
            dma,
        ],
        compiler_params=pltpu.CompilerParams(
            collective_id=0, has_side_effects=True, vmem_limit_bytes=24 * 1024 * 1024
        ),
        name="exchange",
    )(*operands)
    whole = jax.ShapeDtypeStruct((rows_dev, width), jnp.float32)
    return pl.pallas_call(
        finish_kernel,
        out_shape=(whole,) * 3,
        in_specs=[vmem] * 5,
        out_specs=(hbm,) * 3,
        scratch_shapes=[block, dma((4,)), dma((4,)), dma((4,))],
        compiler_params=pltpu.CompilerParams(vmem_limit_bytes=8 * 1024 * 1024),
        name="finish",
    )(weights, update, first, second, row_ratio)


def solution(mesh):
    finer = Mesh(mesh.devices.reshape(4, 2, 4, 2, 2), AXES)
    in_specs = (P(AXES, None), P(AXES, None), P(AXES, None), P(AXES, None), P(), P())
    out_specs = (P(AXES, None), P(AXES, None), P(AXES, None))
    return jax.shard_map(local, mesh=finer, in_specs=in_specs, out_specs=out_specs, check_vma=False)
```
